32 devices in a mesh: dp: 4 (over y, z), ep: 8 (over x, core).
Axes of the slice: x: 4, y: 2, z: 2, core: 2. Of those that a mesh axis runs over, the one named last changes fastest.
The devices are a block of a 4x4x8 slice.
Arguments:
- tokens: bfloat16 [32, 2048, 2048], P(('dp', 'ep')), parts along dimension 0
- w_gate: bfloat16 [2048, 64], replicated
- expert_ids: int32 [32, 2048, 2], P(('dp', 'ep')), parts along dimension 0
- keep_second: int32 [32, 2048], P(('dp', 'ep')), parts along dimension 0
- w_in: bfloat16 [64, 2048, 1024], P('ep')
- w_out: bfloat16 [64, 1024, 2048], P('ep')
Outputs:
- output: bfloat16 [32, 2048, 2048], P(('dp', 'ep')), parts along dimension 0
There are 4 independent parts. The reference program is written for one: setup_inputs(seed, part) draws one part's arguments, and reference() takes and returns one part's arrays. A program takes and returns all parts, laid end to end along the dimension named above; an argument that names none is the same for every part.
All inputs are finite; a program needn't handle non-finite values.
Results may differ from the reference program's by a relative error of at most 0.001.
Values are sent between devices in bfloat16 or wider.
A program may use at most 768 MiB of HBM per device.

```python
import functools
import jax
import jax.numpy as jnp
from jax import lax

GROUPS = 8
TOKENS = 2048
MODEL_DIM = 2048
HIDDEN = 1024
EXPERTS = 64
CAPACITY = 2 * TOKENS // EXPERTS


def draw_routing(route_key):
    k_cover, k_raw, k_shift, k_second, k_keep = jax.random.split(route_key, 5)
    cover_keys = jax.random.split(k_cover, GROUPS)
    cover_ids = jax.vmap(functools.partial(jax.random.permutation, x=EXPERTS))(cover_keys)
    hot_shift = jax.random.randint(k_shift, (), 0, EXPERTS)
    raw_ids = jax.random.randint(k_raw, (GROUPS, TOKENS - EXPERTS), 0, EXPERTS + EXPERTS // 2)
    rest_ids = (raw_ids % EXPERTS + hot_shift) % EXPERTS
    first_ids = jnp.concatenate([cover_ids.astype(jnp.int32), rest_ids.astype(jnp.int32)], axis=1)
    second_ids = (first_ids + jax.random.randint(k_second, (GROUPS, TOKENS), 1, EXPERTS)) % EXPERTS
    keep_second = (jax.random.randint(k_keep, (GROUPS, TOKENS), 0, 10) < 9).astype(jnp.int32)
    expert_ids = jnp.stack([first_ids, second_ids], axis=-1).astype(jnp.int32)
    return expert_ids, keep_second


def setup_inputs(seed: int = 0, part: int = 0) -> dict:
    shared_key, parts_key = jax.random.split(jax.random.key(seed))
    part_key = jax.random.fold_in(parts_key, part)
    k_tokens, k_route = jax.random.split(part_key)
    k_gate, k_in, k_out = jax.random.split(shared_key, 3)
    tokens = jax.random.normal(k_tokens, (GROUPS, TOKENS, MODEL_DIM), jnp.float32).astype(jnp.bfloat16)
    expert_ids, keep_second = draw_routing(k_route)
    w_gate = (jax.random.normal(k_gate, (MODEL_DIM, EXPERTS), jnp.float32) * MODEL_DIM ** -0.5).astype(jnp.bfloat16)
    w_in = (jax.random.normal(k_in, (EXPERTS, MODEL_DIM, HIDDEN), jnp.float32) * MODEL_DIM ** -0.5).astype(jnp.bfloat16)
    w_out = (jax.random.normal(k_out, (EXPERTS, HIDDEN, MODEL_DIM), jnp.float32) * (2.0 / HIDDEN) ** 0.5).astype(jnp.bfloat16)
    return {"tokens": tokens, "w_gate": w_gate, "expert_ids": expert_ids, "keep_second": keep_second, "w_in": w_in, "w_out": w_out}


def group_routing(group_tok, group_ids, group_keep, w_gate):
    logits = jnp.dot(group_tok, w_gate, preferred_element_type=jnp.float32)
    gate_probs = jax.nn.softmax(logits, axis=-1)
    first_hot = jax.nn.one_hot(group_ids[:, 0], EXPERTS, dtype=jnp.int32)
    second_hot = jax.nn.one_hot(group_ids[:, 1], EXPERTS, dtype=jnp.int32) * group_keep[:, None]
    gate_first = jnp.sum(gate_probs * first_hot, axis=-1)
    gate_second = jnp.sum(gate_probs * second_hot, axis=-1)
    gate_total = gate_first + gate_second
    gate_first = gate_first / gate_total
    gate_second = gate_second / gate_total
    pos_first = jnp.sum((jnp.cumsum(first_hot, axis=0) - first_hot) * first_hot, axis=-1)
    second_base = jnp.cumsum(second_hot, axis=0) - second_hot + jnp.sum(first_hot, axis=0)[None, :]
    pos_second = jnp.sum(second_base * second_hot, axis=-1)
    slot_first = first_hot[:, :, None] * jax.nn.one_hot(pos_first, CAPACITY, dtype=jnp.float32)[:, None, :]
    slot_second = second_hot[:, :, None] * jax.nn.one_hot(pos_second, CAPACITY, dtype=jnp.float32)[:, None, :]
    dispatch = slot_first + slot_second
    combine = (gate_first[:, None, None] * slot_first + gate_second[:, None, None] * slot_second).astype(jnp.bfloat16)
    return dispatch, combine


def reference(tokens, w_gate, expert_ids, keep_second, w_in, w_out):
    def dispatch_group(operands):
        group_tok, group_ids, group_keep = operands
        dispatch, _ = group_routing(group_tok, group_ids, group_keep, w_gate)
        sent_rows = jnp.einsum("sec,sm->ecm", dispatch.astype(jnp.float32), group_tok.astype(jnp.float32))
        return sent_rows.astype(jnp.bfloat16)

    expert_in = lax.map(dispatch_group, (tokens, expert_ids, keep_second))
    expert_in = jnp.transpose(expert_in, (1, 0, 2, 3))

    def expert_ffn(operands):
        rows_in, w_first, w_second = operands
        flat_rows = rows_in.reshape(GROUPS * CAPACITY, MODEL_DIM)
        hidden = jax.nn.relu(jnp.dot(flat_rows, w_first, preferred_element_type=jnp.float32)).astype(jnp.bfloat16)
        rows_out = jnp.dot(hidden, w_second, preferred_element_type=jnp.float32).astype(jnp.bfloat16)
        return rows_out.reshape(GROUPS, CAPACITY, MODEL_DIM)

    expert_out = lax.map(expert_ffn, (expert_in, w_in, w_out))
    expert_out = jnp.transpose(expert_out, (1, 0, 2, 3))

    def combine_group(operands):
        group_tok, group_ids, group_keep, rows_back = operands
        _, combine = group_routing(group_tok, group_ids, group_keep, w_gate)
        mixed_rows = jnp.einsum("sec,ecm->sm", combine.astype(jnp.float32), rows_back.astype(jnp.float32))
        return mixed_rows.astype(jnp.bfloat16)

    return lax.map(combine_group, (tokens, expert_ids, keep_second, expert_out))
```

```python
import functools
import jax
import jax.numpy as jnp
from jax import lax
from jax.experimental import pallas as pl
from jax.experimental.pallas import tpu as pltpu
from jax.sharding import PartitionSpec as P

AXIS = "ep"
RING = 3
MESH_ID = pl.DeviceIdType.MESH
BF16 = jnp.bfloat16
F32 = jnp.float32


def tile_of(size, tile):
    return tile if size % tile == 0 else size


def layer_kernel(n, ids_ref, keep_ref, tok_hbm, wg_hbm, wi_hbm, wo_hbm, out_hbm, back_hbm,
                 tok, ring, recv, wi, wo, hid, acc, buf, wg, frow, col,
                 tok_sem, wg_sem, wi_sem, wo_sem, xs_sem, xr_sem, ys_sem, yr_sem, loc_sem, buf_sem, out_sem):
    tokens, dim = tok.shape
    local_experts, rows, _ = recv.shape
    cap = rows // n
    experts = local_experts * n
    hidden = hid.shape[1]
    me = lax.axis_index(AXIS)
    chips = n // 2
    chip, core = me // 2, lax.rem(me, 2)
    steps = sorted(range(chips), key=lambda d: -min(d, chips - d))
    peers = [lax.rem(chip + step, chips) * 2 + lax.rem(core + other, 2)
             for other in (0, 1) for step in steps if (step, other) != (0, 0)]

    barrier = pltpu.get_barrier_semaphore()
    for peer in peers:
        pl.semaphore_signal(barrier, inc=1, device_id={AXIS: peer}, device_id_type=MESH_ID)

    tok_in = pltpu.make_async_copy(tok_hbm.at[0], tok, tok_sem)
    tok_in.start()
    wg_in = pltpu.make_async_copy(wg_hbm, wg, wg_sem)
    wg_in.start()

    def wi_in(e):
        return pltpu.make_async_copy(wi_hbm.at[e], wi, wi_sem)

    def wo_in(e):
        return pltpu.make_async_copy(wo_hbm.at[e], wo, wo_sem)

    wi_in(0).start()
    wo_in(0).start()

    block = tile_of(tokens, 256)
    tri = (lax.broadcasted_iota(jnp.int32, (block, block), 0)
           < lax.broadcasted_iota(jnp.int32, (block, block), 1)).astype(F32).astype(BF16)
    expert_row = lax.broadcasted_iota(jnp.int32, (experts, tokens), 0)
    first_total = jnp.sum((expert_row == ids_ref[0:1, :]).astype(F32), axis=1, keepdims=True)
    expert_blk = lax.broadcasted_iota(jnp.int32, (experts, block), 0)
    carry_1 = jnp.zeros((experts, 1), F32)
    carry_2 = first_total
    for b in range(tokens // block):
        cols = pl.ds(b * block, block)
        id_1, id_2, keep = ids_ref[0:1, cols], ids_ref[1:2, cols], keep_ref[0:1, cols]
        hot_1 = (expert_blk == id_1).astype(F32)
        hot_2 = jnp.where(expert_blk == id_2, keep.astype(F32), 0.0)
        before = jnp.dot(jnp.concatenate([hot_1, hot_2], axis=0).astype(BF16), tri, preferred_element_type=F32)
        pos_1 = jnp.sum(hot_1 * (before[:experts] + carry_1), axis=0, keepdims=True).astype(jnp.int32)
        pos_2 = jnp.sum(hot_2 * (before[experts:] + carry_2), axis=0, keepdims=True).astype(jnp.int32)
        carry_1 = carry_1 + jnp.sum(hot_1, axis=1, keepdims=True)
        carry_2 = carry_2 + jnp.sum(hot_2, axis=1, keepdims=True)
        frow[0:1, cols] = jnp.where(pos_1 < cap, id_1 * cap + pos_1, -1)
        frow[1:2, cols] = jnp.where((keep == 1) & (pos_2 < cap), id_2 * cap + pos_2, -1)
        frow[2:3, cols] = id_1
        frow[3:4, cols] = id_2
        frow[4:5, cols] = keep
        frow[5:8, cols] = jnp.zeros((3, block), jnp.int32)

    tok_in.wait()
    pl.semaphore_wait(barrier, len(peers))

    n_tile = tile_of(dim, 512)
    h_tile = tile_of(hidden, 512)

    def send_x(e, q):
        peer = peers[q]
        return pltpu.make_async_remote_copy(
            src_ref=ring.at[lax.rem(e, RING), pl.ds(pl.multiple_of(peer * cap, cap), cap)],
            dst_ref=recv.at[e, pl.ds(pl.multiple_of(me * cap, cap), cap)],
            send_sem=xs_sem.at[lax.rem(e, RING), q], recv_sem=xr_sem.at[e, q],
            device_id={AXIS: peer}, device_id_type=MESH_ID)

    def send_y(e, q):
        peer = peers[q]
        return pltpu.make_async_remote_copy(
            src_ref=recv.at[e, pl.ds(pl.multiple_of(peer * cap, cap), cap)],
            dst_ref=back_hbm.at[e, pl.ds(pl.multiple_of(me * cap, cap), cap)],
            send_sem=ys_sem.at[e, q], recv_sem=yr_sem.at[e, q],
            device_id={AXIS: peer}, device_id_type=MESH_ID)

    def own_y(e):
        mine = pl.ds(pl.multiple_of(me * cap, cap), cap)
        return pltpu.make_async_copy(recv.at[e, mine], back_hbm.at[e, mine], loc_sem.at[e])

    def dispatch(e):
        slot = lax.rem(e, RING)

        @pl.loop(0, n)
        def _(d):
            place = lax.broadcasted_iota(jnp.int32, (cap, tokens), 0) + (d * local_experts + e) * cap
            hit = (place == frow[0:1, :]) | (place == frow[1:2, :])
            buf[pl.ds(pl.multiple_of(d * cap, cap), cap), :] = hit.astype(F32).astype(BF16)

        @pl.loop(0, dim // n_tile)
        def _(j):
            cols = pl.ds(pl.multiple_of(j * n_tile, n_tile), n_tile)
            ring[slot, :, cols] = jnp.dot(buf[...], tok[:, cols], preferred_element_type=F32).astype(BF16)

        for q in range(len(peers)):
            send_x(e, q).start()
        mine = pl.ds(pl.multiple_of(me * cap, cap), cap)
        recv[e, mine, :] = ring[slot, mine, :]

    @pl.loop(0, RING)
    def _(e):
        dispatch(e)

    lanes = col.shape[1]
    lane = lax.broadcasted_iota(jnp.int32, (lanes, lanes), 1)
    pad = jnp.zeros((lanes - frow.shape[0], lanes), F32)
    for b in range(tokens // lanes):
        cols = pl.ds(b * lanes, lanes)
        col[cols, :] = jnp.transpose(jnp.concatenate([frow[:, cols].astype(F32), pad], axis=0))
    wg_in.wait()
    g_tile = tile_of(tokens, 512)

    @pl.loop(0, tokens // g_tile)
    def _(b):
        part = pl.ds(pl.multiple_of(b * g_tile, g_tile), g_tile)
        logits = jnp.dot(tok[part, :], wg[...], preferred_element_type=F32)
        grown = jnp.exp(logits - jnp.max(logits, axis=-1, keepdims=True))
        probs = grown / jnp.sum(grown, axis=-1, keepdims=True)
        info = col[part, :]
        expert = lax.broadcasted_iota(jnp.int32, (g_tile, experts), 1).astype(F32)
        gate_1 = jnp.sum(jnp.where(expert == info[:, 2:3], probs, 0.0), axis=-1, keepdims=True)
        gate_2 = jnp.sum(jnp.where(expert == info[:, 3:4], probs * info[:, 4:5], 0.0), axis=-1, keepdims=True)
        total = gate_1 + gate_2
        spot = lax.broadcasted_iota(jnp.int32, (g_tile, lanes), 1)
        col[part, :] = jnp.where(spot == 5, gate_1 / total, jnp.where(spot == 6, gate_2 / total, info))

    m_tile = tile_of(tokens, 512)

    @pl.loop(0, tokens // m_tile)
    def _(b):
        acc[pl.ds(pl.multiple_of(b * m_tile, m_tile), m_tile), :] = jnp.zeros((m_tile, dim), F32)

    def weights(e, part):
        info = col[part, :]
        r = lax.broadcasted_iota(jnp.int32, (1, rows), 1)
        place = (r + (r // cap) * ((local_experts - 1) * cap) + e * cap).astype(F32)
        return jnp.where(place == info[:, 0:1], info[:, 5:6],
                         jnp.where(place == info[:, 1:2], info[:, 6:7], 0.0)).astype(BF16)

    def fetch_back(e):
        for q in range(len(peers)):
            send_y(e, q).wait_recv()
        own_y(e).wait()
        load = pltpu.make_async_copy(back_hbm.at[e], buf, buf_sem)
        load.start()
        load.wait()

    def combine(e, last):
        fetch_back(e)

        @pl.loop(0, tokens // m_tile)
        def _(b):
            part = pl.ds(pl.multiple_of(b * m_tile, m_tile), m_tile)
            mix = weights(e, part)

            @pl.loop(0, dim // n_tile)
            def _(j):
                cols = pl.ds(pl.multiple_of(j * n_tile, n_tile), n_tile)
                value = acc[part, cols] + jnp.dot(mix, buf[:, cols], preferred_element_type=F32)
                if last:
                    tok[part, cols] = value.astype(BF16)
                else:
                    acc[part, cols] = value
            if last:
                pltpu.make_async_copy(tok.at[part], out_hbm.at[part], out_sem.at[b]).start()

    @pl.loop(0, local_experts)
    def _(e):
        for q in range(len(peers)):
            send_x(e, q).wait_recv()
        wi_in(e).wait()

        @pl.loop(0, hidden // h_tile)
        def _(j):
            cols = pl.ds(pl.multiple_of(j * h_tile, h_tile), h_tile)
            hid[:, cols] = jnp.maximum(jnp.dot(recv[e], wi[:, cols], preferred_element_type=F32), 0.0).astype(BF16)

        @pl.when(e + 1 < local_experts)
        def _():
            wi_in(e + 1).start()
        wo_in(e).wait()

        @pl.loop(0, dim // n_tile)
        def _(j):
            cols = pl.ds(pl.multiple_of(j * n_tile, n_tile), n_tile)
            recv[e, :, cols] = jnp.dot(hid[...], wo[:, cols], preferred_element_type=F32).astype(BF16)

        @pl.when(e + 1 < local_experts)
        def _():
            wo_in(e + 1).start()
        for q in range(len(peers)):
            send_y(e, q).start()
        own_y(e).start()

        for q in range(len(peers)):
            send_x(e, q).wait_send()

        @pl.when(e + RING < local_experts)
        def _():
            dispatch(e + RING)

        @pl.when(e >= RING)
        def _():
            combine(e - RING, False)

    @pl.loop(local_experts - RING, local_experts - 1)
    def _(e):
        combine(e, False)

    combine(local_experts - 1, True)

    for b in range(tokens // m_tile):
        part = pl.ds(b * m_tile, m_tile)
        pltpu.make_async_copy(tok.at[part], out_hbm.at[part], out_sem.at[b]).wait()

    @pl.loop(0, local_experts)
    def _(e):
        for q in range(len(peers)):
            send_y(e, q).wait_send()


def solution(mesh):
    n = mesh.shape[AXIS]

    def local_layer(tokens, w_gate, expert_ids, keep_second, w_in, w_out):
        token_count, dim = tokens.shape[1:]
        experts = w_gate.shape[1]
        local_experts, _, hidden = w_in.shape
        cap = 2 * token_count // experts
        rows = n * cap
        out, _ = pl.pallas_call(
            functools.partial(layer_kernel, n),
            out_shape=(jax.ShapeDtypeStruct((token_count, dim), BF16),
                       jax.ShapeDtypeStruct((local_experts, rows, dim), BF16)),
            in_specs=[pl.BlockSpec(memory_space=pltpu.VMEM)] * 2 + [pl.BlockSpec(memory_space=pl.ANY)] * 4,
            out_specs=[pl.BlockSpec(memory_space=pl.ANY)] * 2,
            scratch_shapes=[
                pltpu.VMEM((token_count, dim), BF16),
                pltpu.VMEM((RING, rows, dim), BF16),
                pltpu.VMEM((local_experts, rows, dim), BF16),
                pltpu.VMEM((dim, hidden), BF16),
                pltpu.VMEM((hidden, dim), BF16),
                pltpu.VMEM((rows, hidden), BF16),
                pltpu.VMEM((token_count, dim), F32),
                pltpu.VMEM((rows, dim), BF16),
                pltpu.VMEM((dim, experts), BF16),
                pltpu.VMEM((8, token_count), jnp.int32),
                pltpu.VMEM((token_count, 128), F32),
                pltpu.SemaphoreType.DMA,
                pltpu.SemaphoreType.DMA,
                pltpu.SemaphoreType.DMA,
                pltpu.SemaphoreType.DMA,
                pltpu.SemaphoreType.DMA((RING, n - 1)),
                pltpu.SemaphoreType.DMA((local_experts, n - 1)),
                pltpu.SemaphoreType.DMA((local_experts, n - 1)),
                pltpu.SemaphoreType.DMA((local_experts, n - 1)),
                pltpu.SemaphoreType.DMA((local_experts,)),
                pltpu.SemaphoreType.DMA,
                pltpu.SemaphoreType.DMA((token_count // tile_of(token_count, 512),)),
            ],
            compiler_params=pltpu.CompilerParams(collective_id=0, has_side_effects=True,
                                                 vmem_limit_bytes=67_043_328),
        )(expert_ids[0].T, keep_second, tokens, w_gate, w_in, w_out)
        return out[None]

    group_spec = P(("dp", AXIS))
    return jax.shard_map(local_layer, mesh=mesh, in_specs=(group_spec, P(), group_spec, group_spec, P(AXIS), P(AXIS)), out_specs=group_spec, check_vma=False)
```

```python
import functools
import jax
import jax.numpy as jnp
from jax import lax
from jax.experimental import pallas as pl
from jax.experimental.pallas import tpu as pltpu
from jax.sharding import PartitionSpec as P

AXIS = "ep"
RING = 3
MESH_ID = pl.DeviceIdType.MESH
BF16 = jnp.bfloat16
F32 = jnp.float32


def tile_of(size, tile):
    return tile if size % tile == 0 else size


def layer_kernel(n, ids_ref, keep_ref, tok_hbm, wg_hbm, wi_hbm, wo_hbm, tok, back_hbm,
                 ring, recv, wi, wo, hid, acc, buf, last, wg, frow, col,
                 tok_sem, wg_sem, wi_sem, wo_sem, xs_sem, xr_sem, ys_sem, yr_sem, yl_sem, loc_sem, buf_sem):
    tokens, dim = tok.shape
    local_experts, rows, _ = recv.shape
    cap = rows // n
    experts = local_experts * n
    hidden = hid.shape[1]
    me = lax.axis_index(AXIS)
    chips = n // 2
    chip, core = me // 2, lax.rem(me, 2)
    steps = sorted(range(chips), key=lambda d: -min(d, chips - d))
    peers = [lax.rem(chip + step, chips) * 2 + lax.rem(core + other, 2)
             for other in (0, 1) for step in steps if (step, other) != (0, 0)]

    barrier = pltpu.get_barrier_semaphore()
    for peer in peers:
        pl.semaphore_signal(barrier, inc=1, device_id={AXIS: peer}, device_id_type=MESH_ID)

    n_tile = tile_of(dim, 512)
    h_tile = tile_of(hidden, 512)
    n_count = dim // n_tile

    def n_cols(j):
        return pl.ds(pl.multiple_of(j * n_tile, n_tile), n_tile)

    def tok_in(j):
        return pltpu.make_async_copy(tok_hbm.at[0, :, n_cols(j)], tok.at[:, n_cols(j)], tok_sem.at[j])

    for j in range(n_count):
        tok_in(j).start()
    wg_in = pltpu.make_async_copy(wg_hbm, wg, wg_sem)
    wg_in.start()

    def wi_in(e):
        return pltpu.make_async_copy(wi_hbm.at[e], wi, wi_sem)

    def wo_in(e):
        return pltpu.make_async_copy(wo_hbm.at[e], wo, wo_sem)

    block = tile_of(tokens, 256)
    tri = (lax.broadcasted_iota(jnp.int32, (block, block), 0)
           < lax.broadcasted_iota(jnp.int32, (block, block), 1)).astype(F32).astype(BF16)
    expert_row = lax.broadcasted_iota(jnp.int32, (experts, tokens), 0)
    first_total = jnp.sum((expert_row == ids_ref[0:1, :]).astype(F32), axis=1, keepdims=True)
    expert_blk = lax.broadcasted_iota(jnp.int32, (experts, block), 0)
    carry_1 = jnp.zeros((experts, 1), F32)
    carry_2 = first_total
    for b in range(tokens // block):
        cols = pl.ds(b * block, block)
        id_1, id_2, keep = ids_ref[0:1, cols], ids_ref[1:2, cols], keep_ref[0:1, cols]
        hot_1 = (expert_blk == id_1).astype(F32)
        hot_2 = jnp.where(expert_blk == id_2, keep.astype(F32), 0.0)
        before = jnp.dot(jnp.concatenate([hot_1, hot_2], axis=0).astype(BF16), tri, preferred_element_type=F32)
        pos_1 = jnp.sum(hot_1 * (before[:experts] + carry_1), axis=0, keepdims=True).astype(jnp.int32)
        pos_2 = jnp.sum(hot_2 * (before[experts:] + carry_2), axis=0, keepdims=True).astype(jnp.int32)
        carry_1 = carry_1 + jnp.sum(hot_1, axis=1, keepdims=True)
        carry_2 = carry_2 + jnp.sum(hot_2, axis=1, keepdims=True)
        frow[0:1, cols] = jnp.where(pos_1 < cap, id_1 * cap + pos_1, -1)
        frow[1:2, cols] = jnp.where((keep == 1) & (pos_2 < cap), id_2 * cap + pos_2, -1)
        frow[2:3, cols] = id_1
        frow[3:4, cols] = id_2
        frow[4:5, cols] = keep
        frow[5:8, cols] = jnp.zeros((3, block), jnp.int32)

    def send_x(e, q, cols=slice(None)):
        peer = peers[q]
        return pltpu.make_async_remote_copy(
            src_ref=ring.at[lax.rem(e, RING), pl.ds(pl.multiple_of(peer * cap, cap), cap), cols],
            dst_ref=recv.at[e, pl.ds(pl.multiple_of(me * cap, cap), cap), cols],
            send_sem=xs_sem.at[lax.rem(e, RING), q], recv_sem=xr_sem.at[e, q],
            device_id={AXIS: peer}, device_id_type=MESH_ID)

    def send_y(e, q):
        peer = peers[q]
        return pltpu.make_async_remote_copy(
            src_ref=recv.at[e, pl.ds(pl.multiple_of(peer * cap, cap), cap)],
            dst_ref=back_hbm.at[e, pl.ds(pl.multiple_of(me * cap, cap), cap)],
            send_sem=ys_sem.at[e, q], recv_sem=yr_sem.at[e, q],
            device_id={AXIS: peer}, device_id_type=MESH_ID)

    def send_last(j, q):
        peer = peers[q]
        return pltpu.make_async_remote_copy(
            src_ref=recv.at[local_experts - 1, pl.ds(pl.multiple_of(peer * cap, cap), cap), n_cols(j)],
            dst_ref=last.at[pl.ds(pl.multiple_of(me * cap, cap), cap), n_cols(j)],
            send_sem=ys_sem.at[local_experts - 1, q], recv_sem=yl_sem.at[j, q],
            device_id={AXIS: peer}, device_id_type=MESH_ID)

    def own_y(e):
        mine = pl.ds(pl.multiple_of(me * cap, cap), cap)
        return pltpu.make_async_copy(recv.at[e, mine], back_hbm.at[e, mine], loc_sem.at[e])

    mine = pl.ds(pl.multiple_of(me * cap, cap), cap)

    def build_mask(e):
        @pl.loop(0, n)
        def _(d):
            place = lax.broadcasted_iota(jnp.int32, (cap, tokens), 0) + (d * local_experts + e) * cap
            hit = (place == frow[0:1, :]) | (place == frow[1:2, :])
            buf[pl.ds(pl.multiple_of(d * cap, cap), cap), :] = hit.astype(F32).astype(BF16)

    def dispatch(e):
        slot = lax.rem(e, RING)
        build_mask(e)

        @pl.loop(0, n_count)
        def _(j):
            cols = n_cols(j)
            ring[slot, :, cols] = jnp.dot(buf[...], tok[:, cols], preferred_element_type=F32).astype(BF16)

        for q in range(len(peers)):
            send_x(e, q).start()
        recv[e, mine, :] = ring[slot, mine, :]

    build_mask(0)

    @pl.loop(0, n_count)
    def _(j):
        cols = n_cols(j)
        tok_in(j).wait()
        ring[0, :, cols] = jnp.dot(buf[...], tok[:, cols], preferred_element_type=F32).astype(BF16)

        @pl.when(j == 0)
        def _():
            pl.semaphore_wait(barrier, len(peers))
        for q in range(len(peers)):
            send_x(0, q, cols).start()
        recv[0, mine, cols] = ring[0, mine, cols]

    wi_in(0).start()
    wo_in(0).start()

    @pl.loop(1, RING)
    def _(e):
        dispatch(e)

    lanes = col.shape[1]
    lane = lax.broadcasted_iota(jnp.int32, (lanes, lanes), 1)
    pad = jnp.zeros((lanes - frow.shape[0], lanes), F32)
    for b in range(tokens // lanes):
        cols = pl.ds(b * lanes, lanes)
        col[cols, :] = jnp.transpose(jnp.concatenate([frow[:, cols].astype(F32), pad], axis=0))
    wg_in.wait()
    g_tile = tile_of(tokens, 512)

    @pl.loop(0, tokens // g_tile)
    def _(b):
        part = pl.ds(pl.multiple_of(b * g_tile, g_tile), g_tile)
        logits = lax.dot_general(tok[part, :], wg[...], (((1,), (1,)), ((), ())), preferred_element_type=F32)
        grown = jnp.exp(logits - jnp.max(logits, axis=-1, keepdims=True))
        probs = grown / jnp.sum(grown, axis=-1, keepdims=True)
        info = col[part, :]
        expert = lax.broadcasted_iota(jnp.int32, (g_tile, experts), 1).astype(F32)
        gate_1 = jnp.sum(jnp.where(expert == info[:, 2:3], probs, 0.0), axis=-1, keepdims=True)
        gate_2 = jnp.sum(jnp.where(expert == info[:, 3:4], probs * info[:, 4:5], 0.0), axis=-1, keepdims=True)
        total = gate_1 + gate_2
        spot = lax.broadcasted_iota(jnp.int32, (g_tile, lanes), 1)
        col[part, :] = jnp.where(spot == 5, gate_1 / total, jnp.where(spot == 6, gate_2 / total, info))

    m_tile = rows

    @pl.loop(0, tokens // m_tile)
    def _(b):
        acc[pl.ds(pl.multiple_of(b * m_tile, m_tile), m_tile), :] = jnp.zeros((m_tile, dim), F32)

    def weights(e, part):
        info = col[part, :]
        r = lax.broadcasted_iota(jnp.int32, (1, rows), 1)
        place = (r + (r // cap) * ((local_experts - 1) * cap) + e * cap).astype(F32)
        return jnp.where(place == info[:, 0:1], info[:, 5:6],
                         jnp.where(place == info[:, 1:2], info[:, 6:7], 0.0)).astype(BF16)

    def fetch_back(e):
        for q in range(len(peers)):
            send_y(e, q).wait_recv()
        own_y(e).wait()
        load = pltpu.make_async_copy(back_hbm.at[e], buf, buf_sem)
        load.start()
        load.wait()

    def combine(e):
        fetch_back(e)

        @pl.loop(0, tokens // m_tile)
        def _(b):
            part = pl.ds(pl.multiple_of(b * m_tile, m_tile), m_tile)
            mix = weights(e, part)

            @pl.loop(0, n_count)
            def _(j):
                cols = n_cols(j)
                acc[part, cols] += jnp.dot(mix, buf[:, cols], preferred_element_type=F32)

    def expert_hidden(e):
        for q in range(len(peers)):
            send_x(e, q).wait_recv()
        wi_in(e).wait()

        @pl.loop(0, hidden // h_tile)
        def _(j):
            cols = pl.ds(pl.multiple_of(j * h_tile, h_tile), h_tile)
            hid[:, cols] = jnp.maximum(jnp.dot(recv[e], wi[:, cols], preferred_element_type=F32), 0.0).astype(BF16)

    def expert_tile(e, j):
        cols = n_cols(j)
        recv[e, :, cols] = jnp.dot(hid[...], wo[:, cols], preferred_element_type=F32).astype(BF16)

    final = local_experts - 1

    @pl.loop(0, final)
    def _(e):
        expert_hidden(e)
        wi_in(e + 1).start()
        wo_in(e).wait()

        @pl.loop(0, n_count)
        def _(j):
            expert_tile(e, j)

        wo_in(e + 1).start()
        for q in range(len(peers)):
            send_y(e, q).start()
        own_y(e).start()
        for q in range(len(peers)):
            send_x(e, q).wait_send()

        @pl.when(e + RING < local_experts)
        def _():
            dispatch(e + RING)

        @pl.when(e >= RING)
        def _():
            combine(e - RING)

    expert_hidden(final)
    wo_in(final).wait()

    @pl.loop(0, n_count)
    def _(j):
        expert_tile(final, j)
        for q in range(len(peers)):
            send_last(j, q).start()
        last[mine, n_cols(j)] = recv[final, mine, n_cols(j)]

    for q in range(len(peers)):
        send_x(final, q).wait_send()

    @pl.loop(final - RING, final)
    def _(e):
        combine(e)

    @pl.loop(0, tokens // m_tile)
    def _(b):
        part = pl.ds(pl.multiple_of(b * m_tile, m_tile), m_tile)
        buf[:, pl.ds(pl.multiple_of(b * rows, rows), rows)] = weights(final, part)

    @pl.loop(0, n_count)
    def _(j):
        cols = n_cols(j)
        for q in range(len(peers)):
            send_last(j, q).wait_recv()

        @pl.loop(0, tokens // m_tile)
        def _(b):
            part = pl.ds(pl.multiple_of(b * m_tile, m_tile), m_tile)
            mix = buf[:, pl.ds(pl.multiple_of(b * rows, rows), rows)]
            tok[part, cols] = (acc[part, cols] + jnp.dot(mix, last[:, cols], preferred_element_type=F32)).astype(BF16)

    @pl.loop(0, local_experts)
    def _(e):
        for q in range(len(peers)):
            send_y(e, q).wait_send()


def solution(mesh):
    n = mesh.shape[AXIS]

    def local_layer(tokens, w_gate, expert_ids, keep_second, w_in, w_out):
        token_count, dim = tokens.shape[1:]
        experts = w_gate.shape[1]
        local_experts, _, hidden = w_in.shape
        cap = 2 * token_count // experts
        rows = n * cap
        n_count = dim // tile_of(dim, 512)
        result, _ = pl.pallas_call(
            functools.partial(layer_kernel, n),
            out_shape=(pltpu.VMEM((token_count, dim), BF16),
                       jax.ShapeDtypeStruct((local_experts, rows, dim), BF16)),
            in_specs=[pl.BlockSpec(memory_space=pltpu.VMEM)] * 2 + [pl.BlockSpec(memory_space=pl.ANY)] * 4,
            out_specs=[pl.BlockSpec(memory_space=pltpu.VMEM), pl.BlockSpec(memory_space=pl.ANY)],
            scratch_shapes=[
                pltpu.VMEM((RING, rows, dim), BF16),
                pltpu.VMEM((local_experts, rows, dim), BF16),
                pltpu.VMEM((dim, hidden), BF16),
                pltpu.VMEM((hidden, dim), BF16),
                pltpu.VMEM((rows, hidden), BF16),
                pltpu.VMEM((token_count, dim), F32),
                pltpu.VMEM((rows, dim), BF16),
                pltpu.VMEM((rows, dim), BF16),
                pltpu.VMEM((experts, dim), BF16),
                pltpu.VMEM((8, token_count), jnp.int32),
                pltpu.VMEM((token_count, 128), F32),
                pltpu.SemaphoreType.DMA((n_count,)),
                pltpu.SemaphoreType.DMA,
                pltpu.SemaphoreType.DMA,
                pltpu.SemaphoreType.DMA,
                pltpu.SemaphoreType.DMA((RING, n - 1)),
                pltpu.SemaphoreType.DMA((local_experts, n - 1)),
                pltpu.SemaphoreType.DMA((local_experts, n - 1)),
                pltpu.SemaphoreType.DMA((local_experts, n - 1)),
                pltpu.SemaphoreType.DMA((n_count, n - 1)),
                pltpu.SemaphoreType.DMA((local_experts,)),
                pltpu.SemaphoreType.DMA,
            ],
            compiler_params=pltpu.CompilerParams(collective_id=0, has_side_effects=True,
                                                 vmem_limit_bytes=58_195_968),
        )(expert_ids[0].T, keep_second, tokens, w_gate.T, w_in, w_out)
        return result[None]

    group_spec = P(("dp", AXIS))
    return jax.shard_map(local_layer, mesh=mesh, in_specs=(group_spec, P(), group_spec, group_spec, P(AXIS), P(AXIS)), out_specs=group_spec, check_vma=False)
```

```python
import functools
import jax
import jax.numpy as jnp
from jax import lax
from jax.experimental import pallas as pl
from jax.experimental.pallas import tpu as pltpu
from jax.sharding import PartitionSpec as P

AXIS = "ep"
RING = 3
MESH_ID = pl.DeviceIdType.MESH
BF16 = jnp.bfloat16
F32 = jnp.float32


def tile_of(size, tile):
    return tile if size % tile == 0 else size


def layer_kernel(n, ids_hbm, keep_hbm, tok_hbm, wg_hbm, wi_hbm, wo_hbm, tok, back_hbm,
                 ring, recv, wi, wo, hid, acc, buf, last, wg, ids_ref, keep_ref, frow, col,
                 tok_sem, ids_sem, wg_sem, wi_sem, wo_sem, xs_sem, xr_sem, ys_sem, yr_sem, yl_sem, loc_sem, buf_sem):
    tokens, dim = tok.shape
    local_experts, rows, _ = recv.shape
    cap = rows // n
    experts = local_experts * n
    hidden = hid.shape[1]
    me = lax.axis_index(AXIS)
    chips = n // 2
    chip, core = me // 2, lax.rem(me, 2)
    steps = sorted(range(chips), key=lambda d: -min(d, chips - d))
    peers = [lax.rem(chip + step, chips) * 2 + lax.rem(core + other, 2)
             for other in (0, 1) for step in steps if (step, other) != (0, 0)]

    barrier = pltpu.get_barrier_semaphore()
    for peer in peers:
        pl.semaphore_signal(barrier, inc=1, device_id={AXIS: peer}, device_id_type=MESH_ID)

    n_tile = tile_of(dim, 512)
    h_tile = tile_of(hidden, 512)
    n_count = dim // n_tile

    def n_cols(j):
        return pl.ds(pl.multiple_of(j * n_tile, n_tile), n_tile)

    edge = tile_of(n_tile, 256)
    head_cols = [pl.ds(0, edge)] + [pl.ds(edge, n_tile - edge)] * (edge < n_tile)
    tail_cols = [pl.ds(dim - n_tile, n_tile - edge)] * (edge < n_tile) + [pl.ds(dim - edge, edge)]
    heads = len(head_cols) - 1

    def tok_in(j, cols):
        return pltpu.make_async_copy(tok_hbm.at[0, :, cols], tok.at[:, cols], tok_sem.at[j])

    ids_in = pltpu.make_async_copy(ids_hbm, ids_ref, ids_sem.at[0])
    keep_in = pltpu.make_async_copy(keep_hbm, keep_ref, ids_sem.at[1])
    wg_in = pltpu.make_async_copy(wg_hbm, wg, wg_sem)
    ids_in.start()
    keep_in.start()
    tok_in(0, head_cols[0]).start()

    def wi_in(e):
        return pltpu.make_async_copy(wi_hbm.at[e], wi, wi_sem)

    def wo_in(e):
        return pltpu.make_async_copy(wo_hbm.at[e], wo, wo_sem)

    ids_in.wait()
    keep_in.wait()
    for j in range(1, heads + 1):
        tok_in(j, head_cols[j]).start()

    block = tile_of(tokens, 256)
    tri = (lax.broadcasted_iota(jnp.int32, (block, block), 0)
           < lax.broadcasted_iota(jnp.int32, (block, block), 1)).astype(F32).astype(BF16)
    expert_row = lax.broadcasted_iota(jnp.int32, (experts, tokens), 0)
    first_total = jnp.sum((expert_row == ids_ref[0:1, :]).astype(F32), axis=1, keepdims=True)
    expert_blk = lax.broadcasted_iota(jnp.int32, (experts, block), 0)
    carry_1 = jnp.zeros((experts, 1), F32)
    carry_2 = first_total
    for b in range(tokens // block):
        cols = pl.ds(b * block, block)
        id_1, id_2, keep = ids_ref[0:1, cols], ids_ref[1:2, cols], keep_ref[0:1, cols]
        hot_1 = (expert_blk == id_1).astype(F32)
        hot_2 = jnp.where(expert_blk == id_2, keep.astype(F32), 0.0)
        before = jnp.dot(jnp.concatenate([hot_1, hot_2], axis=0).astype(BF16), tri, preferred_element_type=F32)
        pos_1 = jnp.sum(hot_1 * (before[:experts] + carry_1), axis=0, keepdims=True).astype(jnp.int32)
        pos_2 = jnp.sum(hot_2 * (before[experts:] + carry_2), axis=0, keepdims=True).astype(jnp.int32)
        carry_1 = carry_1 + jnp.sum(hot_1, axis=1, keepdims=True)
        carry_2 = carry_2 + jnp.sum(hot_2, axis=1, keepdims=True)
        frow[0:1, cols] = jnp.where(pos_1 < cap, id_1 * cap + pos_1, -1)
        frow[1:2, cols] = jnp.where((keep == 1) & (pos_2 < cap), id_2 * cap + pos_2, -1)
        frow[2:3, cols] = id_1
        frow[3:4, cols] = id_2
        frow[4:5, cols] = keep
        frow[5:8, cols] = jnp.zeros((3, block), jnp.int32)

    def send_x(e, q, cols=slice(None)):
        peer = peers[q]
        return pltpu.make_async_remote_copy(
            src_ref=ring.at[lax.rem(e, RING), pl.ds(pl.multiple_of(peer * cap, cap), cap), cols],
            dst_ref=recv.at[e, pl.ds(pl.multiple_of(me * cap, cap), cap), cols],
            send_sem=xs_sem.at[lax.rem(e, RING)], recv_sem=xr_sem.at[e],
            device_id={AXIS: peer}, device_id_type=MESH_ID)

    def send_y(e, q):
        peer = peers[q]
        return pltpu.make_async_remote_copy(
            src_ref=recv.at[e, pl.ds(pl.multiple_of(peer * cap, cap), cap)],
            dst_ref=back_hbm.at[e, pl.ds(pl.multiple_of(me * cap, cap), cap)],
            send_sem=ys_sem.at[e], recv_sem=yr_sem.at[e],
            device_id={AXIS: peer}, device_id_type=MESH_ID)

    def send_last(j, cols, q):
        peer = peers[q]
        return pltpu.make_async_remote_copy(
            src_ref=recv.at[local_experts - 1, pl.ds(pl.multiple_of(peer * cap, cap), cap), cols],
            dst_ref=last.at[pl.ds(pl.multiple_of(me * cap, cap), cap), cols],
            send_sem=ys_sem.at[local_experts - 1], recv_sem=yl_sem.at[j],
            device_id={AXIS: peer}, device_id_type=MESH_ID)

    away = pl.ds(0, len(peers) * cap)

    def wait_all(sem, cols=slice(None)):
        pltpu.make_async_copy(back_hbm.at[0, away, cols], last.at[away, cols], sem).wait()

    def own_y(e):
        mine = pl.ds(pl.multiple_of(me * cap, cap), cap)
        return pltpu.make_async_copy(recv.at[e, mine], back_hbm.at[e, mine], loc_sem)

    mine = pl.ds(pl.multiple_of(me * cap, cap), cap)

    def build_mask(e):
        @pl.loop(0, n)
        def _(d):
            place = lax.broadcasted_iota(jnp.int32, (cap, tokens), 0) + (d * local_experts + e) * cap
            hit = (place == frow[0:1, :]) | (place == frow[1:2, :])
            buf[pl.ds(pl.multiple_of(d * cap, cap), cap), :] = hit.astype(F32).astype(BF16)

    def dispatch(e):
        slot = lax.rem(e, RING)
        build_mask(e)

        @pl.loop(0, n_count)
        def _(j):
            cols = n_cols(j)
            ring[slot, :, cols] = jnp.dot(buf[...], tok[:, cols], preferred_element_type=F32).astype(BF16)

        for q in range(len(peers)):
            send_x(e, q).start()
        recv[e, mine, :] = ring[slot, mine, :]

    build_mask(0)
    for j in range(1, n_count):
        tok_in(heads + j, n_cols(j)).start()

    def first_out(j, cols):
        tok_in(j, cols).wait()
        half = rows // 2
        for h in (pl.ds(0, half), pl.ds(half, half)):
            ring[0, h, cols] = jnp.dot(buf[h, :], tok[:, cols], preferred_element_type=F32).astype(BF16)
        if isinstance(j, int) and j == 0:
            pl.semaphore_wait(barrier, len(peers))
        for q in range(len(peers)):
            send_x(0, q, cols).start()
        recv[0, mine, cols] = ring[0, mine, cols]

    for j, cols in enumerate(head_cols):
        first_out(j, cols)

    @pl.loop(1, n_count)
    def _(j):
        first_out(j + heads, n_cols(j))

    wi_in(0).start()
    wo_in(0).start()
    wg_in.start()

    @pl.loop(1, RING)
    def _(e):
        dispatch(e)

    lanes = col.shape[1]
    lane = lax.broadcasted_iota(jnp.int32, (lanes, lanes), 1)
    pad = jnp.zeros((lanes - frow.shape[0], lanes), F32)
    for b in range(tokens // lanes):
        cols = pl.ds(b * lanes, lanes)
        col[cols, :] = jnp.transpose(jnp.concatenate([frow[:, cols].astype(F32), pad], axis=0))
    wg_in.wait()
    g_tile = tile_of(tokens, 512)

    @pl.loop(0, tokens // g_tile)
    def _(b):
        part = pl.ds(pl.multiple_of(b * g_tile, g_tile), g_tile)
        logits = lax.dot_general(tok[part, :], wg[...], (((1,), (1,)), ((), ())), preferred_element_type=F32)
        grown = jnp.exp(logits - jnp.max(logits, axis=-1, keepdims=True))
        probs = grown / jnp.sum(grown, axis=-1, keepdims=True)
        info = col[part, :]
        expert = lax.broadcasted_iota(jnp.int32, (g_tile, experts), 1).astype(F32)
        gate_1 = jnp.sum(jnp.where(expert == info[:, 2:3], probs, 0.0), axis=-1, keepdims=True)
        gate_2 = jnp.sum(jnp.where(expert == info[:, 3:4], probs * info[:, 4:5], 0.0), axis=-1, keepdims=True)
        total = gate_1 + gate_2
        spot = lax.broadcasted_iota(jnp.int32, (g_tile, lanes), 1)
        col[part, :] = jnp.where(spot == 5, gate_1 / total, jnp.where(spot == 6, gate_2 / total, info))

    m_tile = rows

    @pl.loop(0, tokens // m_tile)
    def _(b):
        acc[pl.ds(pl.multiple_of(b * m_tile, m_tile), m_tile), :] = jnp.zeros((m_tile, dim), F32)

    def weights(e, part):
        info = col[part, :]
        r = lax.broadcasted_iota(jnp.int32, (1, rows), 1)
        place = (r + (r // cap) * ((local_experts - 1) * cap) + e * cap).astype(F32)
        return jnp.where(place == info[:, 0:1], info[:, 5:6],
                         jnp.where(place == info[:, 1:2], info[:, 6:7], 0.0)).astype(BF16)

    def fetch_back(e):
        wait_all(yr_sem.at[e])
        load = pltpu.make_async_copy(back_hbm.at[e], buf, buf_sem)
        load.start()
        load.wait()

    def combine(e):
        fetch_back(e)

        @pl.loop(0, tokens // m_tile)
        def _(b):
            part = pl.ds(pl.multiple_of(b * m_tile, m_tile), m_tile)
            mix = weights(e, part)

            @pl.loop(0, n_count)
            def _(j):
                cols = n_cols(j)
                acc[part, cols] += jnp.dot(mix, buf[:, cols], preferred_element_type=F32)

    def expert_hidden(e):
        wait_all(xr_sem.at[e])
        wi_in(e).wait()

        @pl.loop(0, hidden // h_tile)
        def _(j):
            cols = pl.ds(pl.multiple_of(j * h_tile, h_tile), h_tile)
            hid[:, cols] = jnp.maximum(jnp.dot(recv[e], wi[:, cols], preferred_element_type=F32), 0.0).astype(BF16)

    def expert_tile(e, cols):
        recv[e, :, cols] = jnp.dot(hid[...], wo[:, cols], preferred_element_type=F32).astype(BF16)

    final = local_experts - 1

    @pl.loop(0, final)
    def _(e):
        expert_hidden(e)
        wi_in(e + 1).start()
        wo_in(e).wait()

        @pl.loop(0, n_count)
        def _(j):
            expert_tile(e, n_cols(j))

        wo_in(e + 1).start()
        for q in range(len(peers)):
            send_y(e, q).start()
        own_y(e).start()
        wait_all(xs_sem.at[lax.rem(e, RING)])

        @pl.when(e + RING < local_experts)
        def _():
            dispatch(e + RING)

        own_y(e).wait()

        @pl.when(e >= RING)
        def _():
            combine(e - RING)

    expert_hidden(final)
    wo_in(final).wait()

    def last_out(j, cols):
        expert_tile(final, cols)
        for q in range(len(peers)):
            send_last(j, cols, q).start()
        last[mine, cols] = recv[final, mine, cols]

    @pl.loop(0, n_count - 1)
    def _(j):
        last_out(j, n_cols(j))

    for k, cols in enumerate(tail_cols):
        last_out(n_count - 1 + k, cols)

    wait_all(xs_sem.at[final % RING])

    @pl.loop(final - RING, final)
    def _(e):
        combine(e)

    @pl.loop(0, tokens // m_tile)
    def _(b):
        part = pl.ds(pl.multiple_of(b * m_tile, m_tile), m_tile)
        buf[:, pl.ds(pl.multiple_of(b * rows, rows), rows)] = weights(final, part)

    def last_in(j, cols):
        wait_all(yl_sem.at[j], cols)

        for b in range(tokens // m_tile):
            part = pl.ds(b * m_tile, m_tile)
            mix = buf[:, pl.ds(b * rows, rows)]
            tok[part, cols] = (acc[part, cols] + jnp.dot(mix, last[:, cols], preferred_element_type=F32)).astype(BF16)

    @pl.loop(0, n_count - 1)
    def _(j):
        last_in(j, n_cols(j))

    for k, cols in enumerate(tail_cols):
        last_in(n_count - 1 + k, cols)

    @pl.loop(0, local_experts)
    def _(e):
        wait_all(ys_sem.at[e])


def solution(mesh):
    n = mesh.shape[AXIS]

    def local_layer(tokens, w_gate, expert_ids, keep_second, w_in, w_out):
        token_count, dim = tokens.shape[1:]
        experts = w_gate.shape[1]
        local_experts, _, hidden = w_in.shape
        cap = 2 * token_count // experts
        rows = n * cap
        n_count = dim // tile_of(dim, 512)
        result, _ = pl.pallas_call(
            functools.partial(layer_kernel, n),
            out_shape=(pltpu.VMEM((token_count, dim), BF16),
                       jax.ShapeDtypeStruct((local_experts, rows, dim), BF16)),
            in_specs=[pl.BlockSpec(memory_space=pl.ANY)] * 6,
            out_specs=[pl.BlockSpec(memory_space=pltpu.VMEM), pl.BlockSpec(memory_space=pl.ANY)],
            scratch_shapes=[
                pltpu.VMEM((RING, rows, dim), BF16),
                pltpu.VMEM((local_experts, rows, dim), BF16),
                pltpu.VMEM((dim, hidden), BF16),
                pltpu.VMEM((hidden, dim), BF16),
                pltpu.VMEM((rows, hidden), BF16),
                pltpu.VMEM((token_count, dim), F32),
                pltpu.VMEM((rows, dim), BF16),
                pltpu.VMEM((rows, dim), BF16),
                pltpu.VMEM((experts, dim), BF16),
                pltpu.VMEM((2, token_count), jnp.int32),
                pltpu.VMEM((1, token_count), jnp.int32),
                pltpu.VMEM((8, token_count), jnp.int32),
                pltpu.VMEM((token_count, 128), F32),
                pltpu.SemaphoreType.DMA((n_count + 1,)),
                pltpu.SemaphoreType.DMA((2,)),
                pltpu.SemaphoreType.DMA,
                pltpu.SemaphoreType.DMA,
                pltpu.SemaphoreType.DMA,
                pltpu.SemaphoreType.DMA((RING,)),
                pltpu.SemaphoreType.DMA((local_experts,)),
                pltpu.SemaphoreType.DMA((local_experts,)),
                pltpu.SemaphoreType.DMA((local_experts,)),
                pltpu.SemaphoreType.DMA((n_count + 1,)),
                pltpu.SemaphoreType.DMA,
                pltpu.SemaphoreType.DMA,
            ],
            compiler_params=pltpu.CompilerParams(collective_id=0, has_side_effects=True,
                                                 vmem_limit_bytes=58_195_968),
        )(expert_ids[0].T, keep_second, tokens, w_gate.T, w_in, w_out)
        return result[None]

    group_spec = P(("dp", AXIS))
    return jax.shard_map(local_layer, mesh=mesh, in_specs=(group_spec, P(), group_spec, group_spec, P(AXIS), P(AXIS)), out_specs=group_spec, check_vma=False)
```

```python
import functools
import jax
import jax.numpy as jnp
from jax import lax
from jax.experimental import pallas as pl
from jax.experimental.pallas import tpu as pltpu
from jax.sharding import PartitionSpec as P

AXIS = "ep"
RING = 3
MESH_ID = pl.DeviceIdType.MESH
BF16 = jnp.bfloat16
F32 = jnp.float32


def tile_of(size, tile):
    return tile if size % tile == 0 else size


def layer_kernel(n, ids_hbm, keep_hbm, tok_hbm, wg_hbm, wi_hbm, wo_hbm, tok, back_hbm,
                 ring, recv, wi, wo, hid, acc, buf, last, wg, ids_ref, keep_ref, frow, col,
                 tok_sem, ids_sem, wg_sem, wi_sem, wo_sem, xs_sem, xr_sem, ys_sem, yr_sem, yl_sem, loc_sem, buf_sem):
    tokens, dim = tok.shape
    local_experts, rows, _ = recv.shape
    cap = rows // n
    experts = local_experts * n
    hidden = hid.shape[1]
    me = lax.axis_index(AXIS)
    chips = n // 2
    chip, core = me // 2, lax.rem(me, 2)
    steps = sorted(range(chips), key=lambda d: -min(d, chips - d))
    peers = [lax.rem(chip + step, chips) * 2 + lax.rem(core + other, 2)
             for other in (0, 1) for step in steps if (step, other) != (0, 0)]

    peer_steps = [step for other in (0, 1) for step in steps if (step, other) != (0, 0)]

    barrier = pltpu.get_barrier_semaphore()
    for peer in peers:
        pl.semaphore_signal(barrier, inc=1, device_id={AXIS: peer}, device_id_type=MESH_ID)

    n_tile = tile_of(dim, 512)
    h_tile = tile_of(hidden, 512)
    n_count = dim // n_tile

    def n_cols(j):
        return pl.ds(pl.multiple_of(j * n_tile, n_tile), n_tile)

    edge = tile_of(n_tile, 256)
    head_cols = [pl.ds(0, edge)] + [pl.ds(edge, n_tile - edge)] * (edge < n_tile)
    tail_cols = [pl.ds(dim - n_tile, n_tile - edge)] * (edge < n_tile) + [pl.ds(dim - edge, edge)]
    heads = len(head_cols) - 1

    def tok_in(j, cols):
        return pltpu.make_async_copy(tok_hbm.at[0, :, cols], tok.at[:, cols], tok_sem.at[j])

    ids_in = pltpu.make_async_copy(ids_hbm, ids_ref, ids_sem.at[0])
    keep_in = pltpu.make_async_copy(keep_hbm, keep_ref, ids_sem.at[1])
    wg_in = pltpu.make_async_copy(wg_hbm, wg, wg_sem)
    ids_in.start()
    keep_in.start()
    tok_in(0, head_cols[0]).start()

    def wi_in(e):
        return pltpu.make_async_copy(wi_hbm.at[e], wi, wi_sem)

    def wo_in(e):
        return pltpu.make_async_copy(wo_hbm.at[e], wo, wo_sem)

    ids_in.wait()
    keep_in.wait()
    for j in range(1, heads + 1):
        tok_in(j, head_cols[j]).start()

    block = tile_of(tokens, 256)
    tri = (lax.broadcasted_iota(jnp.int32, (block, block), 0)
           < lax.broadcasted_iota(jnp.int32, (block, block), 1)).astype(F32).astype(BF16)
    expert_row = lax.broadcasted_iota(jnp.int32, (experts, tokens), 0)
    first_total = jnp.sum((expert_row == ids_ref[0:1, :]).astype(F32), axis=1, keepdims=True)
    expert_blk = lax.broadcasted_iota(jnp.int32, (experts, block), 0)
    carry_1 = jnp.zeros((experts, 1), F32)
    carry_2 = first_total
    for b in range(tokens // block):
        cols = pl.ds(b * block, block)
        id_1, id_2, keep = ids_ref[0:1, cols], ids_ref[1:2, cols], keep_ref[0:1, cols]
        hot_1 = (expert_blk == id_1).astype(F32)
        hot_2 = jnp.where(expert_blk == id_2, keep.astype(F32), 0.0)
        before = jnp.dot(jnp.concatenate([hot_1, hot_2], axis=0).astype(BF16), tri, preferred_element_type=F32)
        pos_1 = jnp.sum(hot_1 * (before[:experts] + carry_1), axis=0, keepdims=True).astype(jnp.int32)
        pos_2 = jnp.sum(hot_2 * (before[experts:] + carry_2), axis=0, keepdims=True).astype(jnp.int32)
        carry_1 = carry_1 + jnp.sum(hot_1, axis=1, keepdims=True)
        carry_2 = carry_2 + jnp.sum(hot_2, axis=1, keepdims=True)
        frow[0:1, cols] = jnp.where(pos_1 < cap, id_1 * cap + pos_1, -1)
        frow[1:2, cols] = jnp.where((keep == 1) & (pos_2 < cap), id_2 * cap + pos_2, -1)
        frow[2:3, cols] = id_1
        frow[3:4, cols] = id_2
        frow[4:5, cols] = keep
        frow[5:8, cols] = jnp.zeros((3, block), jnp.int32)

    def send_x(e, q, cols=slice(None)):
        peer = peers[q]
        return pltpu.make_async_remote_copy(
            src_ref=ring.at[lax.rem(e, RING), pl.ds(pl.multiple_of(peer * cap, cap), cap), cols],
            dst_ref=recv.at[e, pl.ds(pl.multiple_of(me * cap, cap), cap), cols],
            send_sem=xs_sem.at[lax.rem(e, RING)], recv_sem=xr_sem.at[e],
            device_id={AXIS: peer}, device_id_type=MESH_ID)

    def send_y(e, q):
        peer = peers[q]
        return pltpu.make_async_remote_copy(
            src_ref=recv.at[e, pl.ds(pl.multiple_of(peer * cap, cap), cap)],
            dst_ref=back_hbm.at[e, pl.ds(pl.multiple_of(me * cap, cap), cap)],
            send_sem=ys_sem.at[e], recv_sem=yr_sem.at[e],
            device_id={AXIS: peer}, device_id_type=MESH_ID)

    def send_last(j, cols, q):
        peer = peers[q]
        return pltpu.make_async_remote_copy(
            src_ref=recv.at[local_experts - 1, pl.ds(pl.multiple_of(peer * cap, cap), cap), cols],
            dst_ref=last.at[pl.ds(pl.multiple_of(me * cap, cap), cap), cols],
            send_sem=ys_sem.at[local_experts - 1], recv_sem=yl_sem.at[j],
            device_id={AXIS: peer}, device_id_type=MESH_ID)

    away = pl.ds(0, len(peers) * cap)

    def wait_all(sem, cols=slice(None)):
        pltpu.make_async_copy(back_hbm.at[0, away, cols], last.at[away, cols], sem).wait()

    def own_y(e):
        mine = pl.ds(pl.multiple_of(me * cap, cap), cap)
        return pltpu.make_async_copy(recv.at[e, mine], back_hbm.at[e, mine], loc_sem)

    mine = pl.ds(pl.multiple_of(me * cap, cap), cap)

    def build_mask(e):
        @pl.loop(0, n)
        def _(d):
            place = lax.broadcasted_iota(jnp.int32, (cap, tokens), 0) + (d * local_experts + e) * cap
            hit = (place == frow[0:1, :]) | (place == frow[1:2, :])
            buf[pl.ds(pl.multiple_of(d * cap, cap), cap), :] = hit.astype(F32).astype(BF16)

    def dispatch(e):
        slot = lax.rem(e, RING)
        build_mask(e)

        @pl.loop(0, n_count)
        def _(j):
            cols = n_cols(j)
            ring[slot, :, cols] = jnp.dot(buf[...], tok[:, cols], preferred_element_type=F32).astype(BF16)

        for q in range(len(peers)):
            send_x(e, q).start()
        recv[e, mine, :] = ring[slot, mine, :]

    build_mask(0)
    for j in range(1, n_count):
        tok_in(heads + j, n_cols(j)).start()

    def first_out(j, cols):
        tok_in(j, cols).wait()
        parts = steps if isinstance(j, int) and j == 0 else (0,)
        for k, step in enumerate(parts):
            size = rows // len(parts)
            spot = pl.ds(pl.multiple_of(lax.rem(chip + step, len(parts)) * size, size), size)
            ring[0, spot, cols] = jnp.dot(buf[spot, :], tok[:, cols], preferred_element_type=F32).astype(BF16)
            if len(parts) > 1:
                if k == 0:
                    pl.semaphore_wait(barrier, len(peers))
                for q in range(len(peers)):
                    if peer_steps[q] == step:
                        send_x(0, q, cols).start()
        if len(parts) == 1:
            for q in range(len(peers)):
                send_x(0, q, cols).start()
        recv[0, mine, cols] = ring[0, mine, cols]

    for j, cols in enumerate(head_cols):
        first_out(j, cols)

    @pl.loop(1, n_count)
    def _(j):
        first_out(j + heads, n_cols(j))

    wi_in(0).start()
    wo_in(0).start()
    wg_in.start()

    @pl.loop(1, RING)
    def _(e):
        dispatch(e)

    lanes = col.shape[1]
    lane = lax.broadcasted_iota(jnp.int32, (lanes, lanes), 1)
    pad = jnp.zeros((lanes - frow.shape[0], lanes), F32)
    for b in range(tokens // lanes):
        cols = pl.ds(b * lanes, lanes)
        col[cols, :] = jnp.transpose(jnp.concatenate([frow[:, cols].astype(F32), pad], axis=0))
    wg_in.wait()
    g_tile = tile_of(tokens, 512)

    @pl.loop(0, tokens // g_tile)
    def _(b):
        part = pl.ds(pl.multiple_of(b * g_tile, g_tile), g_tile)
        logits = lax.dot_general(tok[part, :], wg[...], (((1,), (1,)), ((), ())), preferred_element_type=F32)
        grown = jnp.exp(logits - jnp.max(logits, axis=-1, keepdims=True))
        probs = grown / jnp.sum(grown, axis=-1, keepdims=True)
        info = col[part, :]
        expert = lax.broadcasted_iota(jnp.int32, (g_tile, experts), 1).astype(F32)
        gate_1 = jnp.sum(jnp.where(expert == info[:, 2:3], probs, 0.0), axis=-1, keepdims=True)
        gate_2 = jnp.sum(jnp.where(expert == info[:, 3:4], probs * info[:, 4:5], 0.0), axis=-1, keepdims=True)
        total = gate_1 + gate_2
        spot = lax.broadcasted_iota(jnp.int32, (g_tile, lanes), 1)
        col[part, :] = jnp.where(spot == 5, gate_1 / total, jnp.where(spot == 6, gate_2 / total, info))

    m_tile = rows

    @pl.loop(0, tokens // m_tile)
    def _(b):
        acc[pl.ds(pl.multiple_of(b * m_tile, m_tile), m_tile), :] = jnp.zeros((m_tile, dim), F32)

    def weights(e, part):
        info = col[part, :]
        r = lax.broadcasted_iota(jnp.int32, (1, rows), 1)
        place = (r + (r // cap) * ((local_experts - 1) * cap) + e * cap).astype(F32)
        return jnp.where(place == info[:, 0:1], info[:, 5:6],
                         jnp.where(place == info[:, 1:2], info[:, 6:7], 0.0)).astype(BF16)

    def fetch_back(e):
        wait_all(yr_sem.at[e])
        load = pltpu.make_async_copy(back_hbm.at[e], buf, buf_sem)
        load.start()
        load.wait()

    def combine(e):
        fetch_back(e)

        @pl.loop(0, tokens // m_tile)
        def _(b):
            part = pl.ds(pl.multiple_of(b * m_tile, m_tile), m_tile)
            mix = weights(e, part)

            @pl.loop(0, n_count)
            def _(j):
                cols = n_cols(j)
                acc[part, cols] += jnp.dot(mix, buf[:, cols], preferred_element_type=F32)

    def expert_hidden(e):
        wait_all(xr_sem.at[e])
        wi_in(e).wait()

        @pl.loop(0, hidden // h_tile)
        def _(j):
            cols = pl.ds(pl.multiple_of(j * h_tile, h_tile), h_tile)
            hid[:, cols] = jnp.maximum(jnp.dot(recv[e], wi[:, cols], preferred_element_type=F32), 0.0).astype(BF16)

    def expert_tile(e, cols):
        recv[e, :, cols] = jnp.dot(hid[...], wo[:, cols], preferred_element_type=F32).astype(BF16)

    final = local_experts - 1

    @pl.loop(0, final)
    def _(e):
        expert_hidden(e)
        wi_in(e + 1).start()
        wo_in(e).wait()

        @pl.loop(0, n_count)
        def _(j):
            expert_tile(e, n_cols(j))

        wo_in(e + 1).start()
        for q in range(len(peers)):
            send_y(e, q).start()
        own_y(e).start()
        wait_all(xs_sem.at[lax.rem(e, RING)])

        @pl.when(e + RING < local_experts)
        def _():
            dispatch(e + RING)

        own_y(e).wait()

        @pl.when(e >= RING)
        def _():
            combine(e - RING)

    expert_hidden(final)
    wo_in(final).wait()

    def last_out(j, cols):
        expert_tile(final, cols)
        for q in range(len(peers)):
            send_last(j, cols, q).start()
        last[mine, cols] = recv[final, mine, cols]

    @pl.loop(0, n_count - 1)
    def _(j):
        last_out(j, n_cols(j))

    for k, cols in enumerate(tail_cols):
        last_out(n_count - 1 + k, cols)

    wait_all(xs_sem.at[final % RING])

    @pl.loop(final - RING, final)
    def _(e):
        combine(e)

    @pl.loop(0, tokens // m_tile)
    def _(b):
        part = pl.ds(pl.multiple_of(b * m_tile, m_tile), m_tile)
        buf[:, pl.ds(pl.multiple_of(b * rows, rows), rows)] = weights(final, part)

    def last_in(j, cols):
        wait_all(yl_sem.at[j], cols)

        for b in range(tokens // m_tile):
            part = pl.ds(b * m_tile, m_tile)
            mix = buf[:, pl.ds(b * rows, rows)]
            tok[part, cols] = (acc[part, cols] + jnp.dot(mix, last[:, cols], preferred_element_type=F32)).astype(BF16)

    @pl.loop(0, n_count - 1)
    def _(j):
        last_in(j, n_cols(j))

    for k, cols in enumerate(tail_cols):
        last_in(n_count - 1 + k, cols)

    @pl.loop(0, local_experts)
    def _(e):
        wait_all(ys_sem.at[e])


def solution(mesh):
    n = mesh.shape[AXIS]

    def local_layer(tokens, w_gate, expert_ids, keep_second, w_in, w_out):
        token_count, dim = tokens.shape[1:]
        experts = w_gate.shape[1]
        local_experts, _, hidden = w_in.shape
        cap = 2 * token_count // experts
        rows = n * cap
        n_count = dim // tile_of(dim, 512)
        result, _ = pl.pallas_call(
            functools.partial(layer_kernel, n),
            out_shape=(pltpu.VMEM((token_count, dim), BF16),
                       jax.ShapeDtypeStruct((local_experts, rows, dim), BF16)),
            in_specs=[pl.BlockSpec(memory_space=pl.ANY)] * 6,
            out_specs=[pl.BlockSpec(memory_space=pltpu.VMEM), pl.BlockSpec(memory_space=pl.ANY)],
            scratch_shapes=[
                pltpu.VMEM((RING, rows, dim), BF16),
                pltpu.VMEM((local_experts, rows, dim), BF16),
                pltpu.VMEM((dim, hidden), BF16),
                pltpu.VMEM((hidden, dim), BF16),
                pltpu.VMEM((rows, hidden), BF16),
                pltpu.VMEM((token_count, dim), F32),
                pltpu.VMEM((rows, dim), BF16),
                pltpu.VMEM((rows, dim), BF16),
                pltpu.VMEM((experts, dim), BF16),
                pltpu.VMEM((2, token_count), jnp.int32),
                pltpu.VMEM((1, token_count), jnp.int32),
                pltpu.VMEM((8, token_count), jnp.int32),
                pltpu.VMEM((token_count, 128), F32),
                pltpu.SemaphoreType.DMA((n_count + 1,)),
                pltpu.SemaphoreType.DMA((2,)),
                pltpu.SemaphoreType.DMA,
                pltpu.SemaphoreType.DMA,
                pltpu.SemaphoreType.DMA,
                pltpu.SemaphoreType.DMA((RING,)),
                pltpu.SemaphoreType.DMA((local_experts,)),
                pltpu.SemaphoreType.DMA((local_experts,)),
                pltpu.SemaphoreType.DMA((local_experts,)),
                pltpu.SemaphoreType.DMA((n_count + 1,)),
                pltpu.SemaphoreType.DMA,
                pltpu.SemaphoreType.DMA,
            ],
            compiler_params=pltpu.CompilerParams(collective_id=0, has_side_effects=True,
                                                 vmem_limit_bytes=58_195_968),
        )(expert_ids[0].T, keep_second, tokens, w_gate.T, w_in, w_out)
        return result[None]

    group_spec = P(("dp", AXIS))
    return jax.shard_map(local_layer, mesh=mesh, in_specs=(group_spec, P(), group_spec, group_spec, P(AXIS), P(AXIS)), out_specs=group_spec, check_vma=False)
```
